32 devices in a mesh: rep: 1, r: 8 (over y, z), s: 4 (over x, core).
Axes of the slice: x: 2, y: 2, z: 4, core: 2. Of those that a mesh axis runs over, the one named last changes fastest.
Arguments:
- x: bfloat16 [32, 4096, 640], P(('rep', 'r', 's'))
- dy: bfloat16 [32, 4096, 640], P(('rep', 'r', 's'))
- w_gate: bfloat16 [2, 640, 2048], P(None, 's')
- w_up: bfloat16 [2, 640, 2048], P(None, 's')
- w_down: bfloat16 [2, 2048, 640], P(None, 's')
- m_w_gate: float32 [2, 640, 2048], P(None, 's')
- m_w_up: float32 [2, 640, 2048], P(None, 's')
- m_w_down: float32 [2, 2048, 640], P(None, 's')
- v_w_gate: float32 [2, 640, 2048], P(None, 's')
- v_w_up: float32 [2, 640, 2048], P(None, 's')
- v_w_down: float32 [2, 2048, 640], P(None, 's')
Outputs:
- output 1: bfloat16 [2, 640, 2048], P('rep', 's')
- output 2: bfloat16 [2, 640, 2048], P('rep', 's')
- output 3: bfloat16 [2, 2048, 640], P('rep', 's')
- output 4: float32 [2, 640, 2048], P('rep', 's')
- output 5: float32 [2, 640, 2048], P('rep', 's')
- output 6: float32 [2, 2048, 640], P('rep', 's')
- output 7: float32 [2, 640, 2048], P('rep', 's')
- output 8: float32 [2, 640, 2048], P('rep', 's')
- output 9: float32 [2, 2048, 640], P('rep', 's')
All inputs are finite; a program needn't handle non-finite values.
Results may differ from the reference program's by a relative error of at most 0.022.
Values are sent between devices in bfloat16 or wider.
A program may use at most 2 GiB of HBM per device.

```python
import jax
import jax.numpy as jnp
from jax import lax

SEQUENCES = 32
TOKENS = 4096
D = 640
FF = 2048
LAYERS = 2
NAMES = ("w_gate", "w_up", "w_down")
SHAPES = {"w_gate": (LAYERS, D, FF), "w_up": (LAYERS, D, FF), "w_down": (LAYERS, FF, D)}


def bump(key, n, height):
    away = (jnp.arange(n, dtype=jnp.int32) - jax.random.randint(key, (), 0, n, jnp.int32)) % n
    return jnp.where(away < n // 8, height, 1.0)


def together(key, own, strength):
    shared = jax.random.normal(key, own.shape[1:], jnp.float32)
    return (own + strength * shared) * lax.rsqrt(1 + strength * strength)


def setup_inputs(seed: int = 0, part: int = 0) -> dict:
    kx, kdy, ka, kb, kz, kf, kh, kl, *keys = jax.random.split(jax.random.key(seed), 8 + 3 * len(NAMES))
    kx, kdy, ka, kb = (jax.random.fold_in(k, part) for k in (kx, kdy, ka, kb))
    kw, km, kv = (keys[i::3] for i in range(3))
    shape = (SEQUENCES, TOKENS, D)
    much_x, much_dy = jax.random.uniform(kz, (2,), jnp.float32, 0.0, 1.0)
    loud = 2.0 ** jax.random.uniform(jax.random.fold_in(kz, 1), (), jnp.float32, -1.0, 2.0)
    layers = 2.0 ** jax.random.uniform(kl, (LAYERS, 1, 1), jnp.float32, -1.0, 1.0)
    x = together(ka, jax.random.normal(kx, shape, jnp.float32), much_x) * bump(kf, D, 4.0)
    dy = together(kb, jax.random.normal(kdy, shape, jnp.float32), much_dy)
    drawn = {"x": x.astype(jnp.bfloat16), "dy": (loud * dy * (SEQUENCES * TOKENS) ** -0.5).astype(jnp.bfloat16)}
    for key, name in zip(kw, NAMES, strict=True):
        w = jax.random.normal(key, SHAPES[name], jnp.float32) * SHAPES[name][1] ** -0.5
        drawn[name] = (w * {"w_gate": 1.0, "w_up": bump(kh, FF, 4.0), "w_down": layers}[name]).astype(jnp.bfloat16)
    for key, name in zip(km, NAMES, strict=True):
        drawn[f"m_{name}"] = 0.1 * jax.random.normal(key, SHAPES[name], jnp.float32)
    for key, name in zip(kv, NAMES, strict=True):
        drawn[f"v_{name}"] = jax.random.uniform(key, SHAPES[name], jnp.float32, 0.005, 0.015)
    return drawn


def matmul(a, w):
    return jnp.dot(a, w, preferred_element_type=jnp.float32).astype(jnp.bfloat16)


def normed(h):
    wide = h.astype(jnp.float32)
    scale = lax.rsqrt(jnp.mean(wide**2, -1, keepdims=True) + 1e-6)
    return (wide * scale).astype(jnp.bfloat16)


def layer(h, w):
    a = normed(h)
    gate = jnp.dot(a, w["w_gate"], preferred_element_type=jnp.float32)
    up = jnp.dot(a, w["w_up"], preferred_element_type=jnp.float32)
    return h + matmul((jax.nn.silu(gate) * up).astype(jnp.bfloat16), w["w_down"])


def adamw(w, m, v, g):
    m = 0.9 * m + 0.1 * g
    v = 0.95 * v + 0.05 * g * g
    step = m * lax.rsqrt(v + 1e-8) + 0.1 * w
    return (w - 0.02 * step).astype(jnp.bfloat16), m, v


def clipped(gradients, sum_of_squares, count):
    factor = jnp.minimum(1.0, 0.5 * lax.rsqrt(sum_of_squares / count + 1e-30))
    return [g * factor for g in gradients]


def stack(weights, h):
    return lax.scan(lambda h, w: (layer(h, w), None), h, weights)[0]


def reference(x, dy, w_gate, w_up, w_down, m_w_gate, m_w_up, m_w_down, v_w_gate, v_w_up, v_w_down):
    weights = dict(zip(NAMES, (w_gate, w_up, w_down), strict=True))

    def take(so_far, sequence):
        h, by_y = sequence
        _, back = jax.vjp(lambda w: stack(w, h), weights)
        return jax.tree.map(lambda total, term: total + term.astype(jnp.float32), so_far, back(by_y)[0]), None

    none_yet = {name: jnp.zeros(w.shape, jnp.float32) for name, w in weights.items()}
    by_weights, _ = lax.scan(take, none_yet, (x, dy))
    gradients = [by_weights[name].astype(jnp.bfloat16).astype(jnp.float32) for name in NAMES]
    gradients = clipped(gradients, sum(jnp.sum(g * g) for g in gradients), sum(g.size for g in gradients))
    new = [
        adamw(w.astype(jnp.float32), m, v, g)
        for w, m, v, g in zip((w_gate, w_up, w_down), (m_w_gate, m_w_up, m_w_down), (v_w_gate, v_w_up, v_w_down), gradients, strict=True)
    ]
    return tuple(one[which] for which in range(3) for one in new)
```

```python
import functools

import jax
import jax.numpy as jnp
from jax import lax
from jax.experimental import pallas as pl
from jax.experimental.pallas import tpu as pltpu
from jax.sharding import PartitionSpec as P

F32, BF16 = jnp.float32, jnp.bfloat16
MESH = pl.DeviceIdType.MESH
LIMIT = 66_000_000
NT = (((1,), (1,)), ((), ()))
TOKENS_F, TOKENS_B = 512, 1024
LANES, WIDE, HALF, OWN = 128, 512, 240, 160
THREE = range(3)
STEPS_Z = (1, 2, 3)


def dot(a, b):
    return jnp.dot(a, b, preferred_element_type=F32)


def dot_nt(a, b):
    return lax.dot_general(a, b, NT, preferred_element_type=F32)


def sigmoid(g):
    return 0.5 * jnp.tanh(0.5 * g) + 0.5


def scale_of(wide):
    return lax.rsqrt(jnp.mean(wide * wide, -1, keepdims=True) + 1e-6)


def keep(ref, value, q):
    for c in range(4):
        ref[0, c, :, LANES * q : LANES * q + LANES] = value[:, LANES * c : LANES * c + LANES]


def forward_kernel(x_ref, g_block, u_block, d_block, h_ref, at_ref, g_ref, u_ref, wg_all, wu_all, wd_all, z_ref, *scratch):
    own, held, sems_s, sems_r, sems_own, sems_held = scratch[:3], scratch[3:6], *scratch[6:]
    step, steps = pl.program_id(0), pl.num_programs(0)
    rep, r, s = lax.axis_index("rep"), lax.axis_index("r"), lax.axis_index("s")
    ax, core, ay, az = s // 2, s % 2, r // 4, r % 4
    mate = (rep, r, ax * 2 + 1 - core)
    far = (1 - ax) * 2 + core
    across = (rep, r, far)
    over = (rep, (1 - ay) * 4 + az, s)
    blocks, alls, halves = (g_block, u_block, d_block), (wg_all, wu_all, wd_all), (80, 80, 256)

    def half(i, layer, place, which):
        n = halves[i]
        return alls[i].at[layer, pl.ds(pl.multiple_of(2 * n * place + n * which, 16), n)]

    def copy(kind, i, layer, src, dst, who):
        return pltpu.make_async_remote_copy(
            src_ref=src,
            dst_ref=dst,
            send_sem=sems_s.at[kind, layer, i],
            recv_sem=sems_r.at[kind, layer, i],
            device_id=who,
            device_id_type=MESH,
        )

    def whole_block(i, layer, place):
        n = 2 * halves[i]
        return alls[i].at[layer, pl.ds(pl.multiple_of(n * place, 16), n)]

    def to_mate(i, layer):
        return copy(0, i, layer, blocks[i].at[layer], whole_block(i, layer, s), mate)

    def to_across(i, layer):
        n = halves[i]
        return copy(1, i, layer, blocks[i].at[layer, pl.ds(pl.multiple_of(n * ay, 16), n)], half(i, layer, s, ay), across)

    def to_over(i, layer):
        return copy(2, i, layer, half(i, layer, far, ay), half(i, layer, far, ay), over)

    def near_on(i, layer):
        return copy(3, i, layer, half(i, layer, far, ay), half(i, layer, far, ay), mate)

    def far_on(i, layer):
        return copy(4, i, layer, half(i, layer, far, 1 - ay), half(i, layer, far, 1 - ay), mate)

    def own_in(i, layer):
        return pltpu.make_async_copy(blocks[i].at[layer], own[i].at[layer], sems_own.at[0, layer, i])

    def own_out(i, layer):
        return pltpu.make_async_copy(own[i].at[layer], whole_block(i, layer, s), sems_own.at[1, layer, i])

    def first_half(layer):
        for i in THREE:
            to_across(i, layer).wait_recv()
            to_over(i, layer).start()
            near_on(i, layer).start()

    def second_half(layer):
        for i in THREE:
            to_over(i, layer).wait_recv()
            far_on(i, layer).start()

    def finish(layer):
        for i in THREE:
            to_across(i, layer).wait_send()
            to_over(i, layer).wait_send()
            to_mate(i, layer).wait()
            near_on(i, layer).wait()
            far_on(i, layer).wait()
            own_out(i, layer).wait()

    @pl.when(step == 0)
    def _():
        for layer in range(2):
            for i in THREE:
                own_in(i, layer).start()
        barrier = pltpu.get_barrier_semaphore()
        for who in (mate, across, over):
            pl.semaphore_signal(barrier, inc=1, device_id=who, device_id_type=MESH)
        pl.semaphore_wait(barrier, 3)
        for layer in range(2):
            for i in THREE:
                to_across(i, layer).start()
        for layer in range(2):
            for i in THREE:
                to_mate(i, layer).start()
                own_in(i, layer).wait()
                own_out(i, layer).start()
        first_half(0)
        second_half(0)
        finish(0)
        loads = [pltpu.make_async_copy(alls[i].at[0], held[i], sems_held.at[i]) for i in THREE]
        for load in loads:
            load.start()
        for load in loads:
            load.wait()

    @pl.when(step == 1)
    def _():
        first_half(1)

    @pl.when(step == 3)
    def _():
        second_half(1)

    @pl.when(step == steps - 1)
    def _():
        finish(1)

    wg_ref, wu_ref, wd_ref = held
    x = x_ref[...]
    wide = x.astype(F32)
    a = (wide * scale_of(wide)).astype(BF16)
    at_ref[0] = a.T
    for q in range(4):
        cols = slice(WIDE * q, WIDE * q + WIDE)
        gate = dot(a, wg_ref[:, cols])
        up = dot(a, wu_ref[:, cols])
        keep(g_ref, gate, q)
        keep(u_ref, up, q)
        z_ref[:, cols] = (gate * sigmoid(gate) * up).astype(BF16)
    out = dot(z_ref[...], wd_ref[...]).astype(BF16)
    h_ref[...] = (wide + out.astype(F32)).astype(BF16)


def grads(gate, up, dz):
    s = sigmoid(gate)
    silu = gate * s
    dup = dz * silu
    dgate = dz * up * (s + silu * (1.0 - s))
    return silu * up, dgate, dup


def turn_kernel(h_ref, dy_ref, wg_ref, wu_ref, wd_ref, at_in, g_in, u_in, dys_ref, dyt_ref, at_ref, g_ref, u_ref, dg_ref, du_ref):
    wide = h_ref[...].astype(F32)
    scale = scale_of(wide)
    a = (wide * scale).astype(BF16)
    at_ref[0] = a.T
    dy = dy_ref[...]
    for q in range(4):
        cols = slice(WIDE * q, WIDE * q + WIDE)
        gate = dot(a, wg_ref[:, cols])
        up = dot(a, wu_ref[:, cols])
        dz = dot_nt(dy, wd_ref[cols, :]).astype(BF16).astype(F32)
        keep(g_ref, gate, q)
        keep(u_ref, up, q)
        _, dgate, dup = grads(gate, up, dz)
        dg_ref[:, cols] = dgate.astype(BF16)
        du_ref[:, cols] = dup.astype(BF16)
    da = dot_nt(dg_ref[...], wg_ref[...]) + dot_nt(du_ref[...], wu_ref[...])
    dot_mean = jnp.mean(da * wide, -1, keepdims=True)
    dh = da * scale - wide * (scale * scale * scale * dot_mean)
    dh = (dy.astype(F32) + dh).astype(BF16)
    dys_ref[1] = dy
    dys_ref[0] = dh
    dyt_ref[1] = dy.T
    dyt_ref[0] = dh.T


def forward(x, wg, wu, wd):
    n, d = x.shape
    f = wg.shape[2]
    t = TOKENS_F
    row = pl.BlockSpec((t, d), lambda i: (i, 0))
    kept = pl.BlockSpec((1, 4, t, f // 4), lambda i: (0, 0, i, 0))
    hbm = pl.BlockSpec(memory_space=pl.ANY)
    return pl.pallas_call(
        forward_kernel,
        grid=(n // t,),
        in_specs=[row, hbm, hbm, hbm],
        out_specs=[row, pl.BlockSpec((1, d, t), lambda i: (0, 0, i)), kept, kept, hbm, hbm, hbm],
        out_shape=[
            jax.ShapeDtypeStruct((n, d), BF16),
            jax.ShapeDtypeStruct((2, d, n), BF16),
            jax.ShapeDtypeStruct((2, 4, n, f // 4), F32),
            jax.ShapeDtypeStruct((2, 4, n, f // 4), F32),
            jax.ShapeDtypeStruct((2, d, f), BF16),
            jax.ShapeDtypeStruct((2, d, f), BF16),
            jax.ShapeDtypeStruct((2, f, d), BF16),
        ],
        scratch_shapes=[
            pltpu.VMEM((t, f), BF16),
            *[pltpu.VMEM(w.shape, BF16) for w in (wg, wu, wd)],
            pltpu.VMEM((d, f), BF16),
            pltpu.VMEM((d, f), BF16),
            pltpu.VMEM((f, d), BF16),
            pltpu.SemaphoreType.DMA((5, 2, 3)),
            pltpu.SemaphoreType.DMA((5, 2, 3)),
            pltpu.SemaphoreType.DMA((2, 2, 3)),
            pltpu.SemaphoreType.DMA((3,)),
        ],
        compiler_params=pltpu.CompilerParams(vmem_limit_bytes=LIMIT, collective_id=0, has_side_effects=True),
        cost_estimate=pl.CostEstimate(flops=6 * n * d * f, bytes_accessed=100_000_000, transcendentals=0),
        name="forward",
    )(x, wg, wu, wd)


def turn(h, dy, wg, wu, wd, at, g, u):
    n, d = h.shape
    f = wg.shape[2]
    t = TOKENS_F
    whole = lambda s: pl.BlockSpec((None, *s), lambda i: (1, 0, 0), pipeline_mode=pl.Buffered(1))
    row = pl.BlockSpec((t, d), lambda i: (i, 0))
    kept = pl.BlockSpec((1, 4, t, f // 4), lambda i: (1, 0, i, 0))
    hbm = pl.BlockSpec(memory_space=pl.ANY)
    return pl.pallas_call(
        turn_kernel,
        grid=(n // t,),
        in_specs=[row, row, whole((d, f)), whole((d, f)), whole((f, d)), hbm, hbm, hbm],
        out_specs=[
            pl.BlockSpec((2, t, d), lambda i: (0, i, 0)),
            pl.BlockSpec((2, d, t), lambda i: (0, 0, i)),
            pl.BlockSpec((1, d, t), lambda i: (1, 0, i)),
            kept,
            kept,
        ],
        out_shape=[
            jax.ShapeDtypeStruct((2, n, d), BF16),
            jax.ShapeDtypeStruct((2, d, n), BF16),
            jax.ShapeDtypeStruct((2, d, n), BF16),
            jax.ShapeDtypeStruct((2, 4, n, f // 4), F32),
            jax.ShapeDtypeStruct((2, 4, n, f // 4), F32),
        ],
        input_output_aliases={5: 2, 6: 3, 7: 4},
        scratch_shapes=[pltpu.VMEM((t, f), BF16)] * 2,
        compiler_params=pltpu.CompilerParams(vmem_limit_bytes=LIMIT),
        cost_estimate=pl.CostEstimate(flops=10 * n * d * f, bytes_accessed=100_000_000, transcendentals=0),
        name="turn",
    )(h, dy, wg, wu, wd, at, g, u)


TICKS = 4
PIECES = 4
t_b = TOKENS_B // PIECES
CHUNKS = 8


def sum_kernel(dys_ref, dyt_ref, at_ref, g_ref, u_ref, wd_ref, out_ref, sq_ref, acc, p, rc, q, rx, sy, ry, sz, rz, sems_s, sems_r, zs, dgs, dus, sqz, sqp, sqr, sq_s, sq_r, fin, fin_s):
    tick = pl.program_id(0)
    chunk, part = tick // TICKS, tick % TICKS
    rep, r, s = lax.axis_index("rep"), lax.axis_index("r"), lax.axis_index("s")
    x, core, y, z = s // 2, s % 2, r // 4, r % 4
    mate = (rep, r, x * 2 + 1 - core)
    across = (rep, r, (1 - x) * 2 + core)
    over = (rep, (1 - y) * 4 + z, s)
    others = [(rep, y * 4 + (z + k) % 4, s) for k in STEPS_Z]

    @pl.when(tick == 0)
    def _():
        barrier = pltpu.get_barrier_semaphore()
        for who in [mate, across, over, *others]:
            pl.semaphore_signal(barrier, inc=1, device_id=who, device_id_type=MESH)
        pl.semaphore_wait(barrier, 6)
        sq_ref[...] = jnp.zeros_like(sq_ref)

    def copy(src, dst, kind, j, who):
        return pltpu.make_async_remote_copy(
            src_ref=src, dst_ref=dst, send_sem=sems_s.at[kind, j], recv_sem=sems_r.at[kind, j], device_id=who, device_id_type=MESH
        )

    def by_core(j):
        return copy(p.at[j % 2, 1 - core], rc.at[j], 0, j, mate)

    def by_x(j):
        return copy(q.at[j % 2, 1 - x], rx.at[j], 1, j, across)

    def by_y(j):
        return copy(sy.at[j % 2, 1 - y], ry.at[j], 2, j, over)

    def by_z(j, k):
        return copy(sz.at[j % 2, (z + k) % 4], rz.at[j, k - 1], 2 + k, j, others[k - 1])

    def all_z(j, k):
        return copy(fin.at[j, y, z], fin.at[j, y, z], 5 + k, j, others[k - 1])

    def all_y(j):
        return copy(fin.at[j, y], fin.at[j, y], 9, j, over)

    def square(src, dst, kind, who):
        return pltpu.make_async_remote_copy(
            src_ref=src, dst_ref=dst, send_sem=sq_s.at[kind], recv_sem=sq_r.at[kind], device_id=who, device_id_type=MESH
        )

    def squares_z(k):
        return square(sqz.at[z], sqz.at[z], k - 1, others[k - 1])

    def squares(k):
        return square(sqp.at[k], sqr.at[k], 3 + k, (over, across, mate)[k])

    def give(j):
        return pltpu.make_async_copy(fin.at[j], out_ref.at[j], fin_s.at[j])

    def at(rounds, when, j_ok=True):
        j = chunk - rounds
        return j, (part == when) & (j >= 0) & (j < CHUNKS)

    j, now = at(1, 0)

    @pl.when(now)
    def _():
        by_core(j).wait()
        for k in range(2):
            q[j % 2, k] = (p[j % 2, core, k].astype(F32) + rc[j, k].astype(F32)).astype(BF16)
        by_x(j).start()

    j, now = at(2, 0)

    @pl.when(now)
    def _():
        by_x(j).wait()
        total = (q[j % 2, x].astype(F32) + rx[j].astype(F32)).astype(BF16)
        for k in range(2):
            for i in range(4):
                sy[j % 2, k, i] = total[HALF * k : HALF * k + HALF, LANES * i : LANES * i + LANES]
        by_y(j).start()

    j, now = at(2, 2)

    @pl.when(now)
    def _():
        by_y(j).wait()
        sz[j % 2] = (sy[j % 2, y].astype(F32) + ry[j].astype(F32)).astype(BF16)
        for k in STEPS_Z:
            by_z(j, k).start()

    j, now = at(3, 0)

    @pl.when(now)
    def _():
        for k in STEPS_Z:
            by_z(j, k).wait()
        total = sz[j % 2, z].astype(F32)
        for k in THREE:
            total += rz[j, k].astype(F32)
        total = total.astype(BF16)
        fin[j, y, z] = total
        total = total.astype(F32)
        sq_ref[...] += jnp.sum((total * total).reshape(30, 8, LANES), 0)
        for k in STEPS_Z:
            all_z(j, k).start()

        @pl.when(j == CHUNKS - 1)
        def _():
            sqz[z] = sq_ref[...]
            for k in STEPS_Z:
                squares_z(k).start()

    j, now = at(3, 2)

    @pl.when(now)
    def _():
        for k in STEPS_Z:
            all_z(j, k).wait()
        all_y(j).start()

        @pl.when(j == CHUNKS - 1)
        def _():
            for k in STEPS_Z:
                squares_z(k).wait()
            total = (sqz[0] + sqz[1]) + (sqz[2] + sqz[3])
            for k in THREE:
                sqp[k] = total
                squares(k).start()
                squares(k).wait()
                total = total + sqr[k]
            sq_ref[...] = total

    j, now = at(4, 0)

    @pl.when(now)
    def _():
        all_y(j).wait()
        give(j).start()

    @pl.when(tick == pl.num_programs(0) - 1)
    def _():
        for j in range(CHUNKS):
            give(j).wait()

    @pl.when(chunk < CHUNKS)
    def _():
        @pl.when(part == 0)
        def _():
            acc[...] = jnp.zeros_like(acc)

        w = wd_ref[0, :, 0].reshape(WIDE, 640)
        for i in range(PIECES):
            rows = slice(t_b * i, t_b * i + t_b)
            dz = dot_nt(dys_ref[0, rows], w).astype(BF16).astype(F32)
            for ref, value in zip((zs, dgs, dus), grads(g_ref[0, 0, rows], u_ref[0, 0, rows], dz), strict=True):
                ref[rows] = value.astype(BF16)
        acc[0] += dot(at_ref[0], dgs[...])
        acc[1] += dot(at_ref[0], dus[...])
        acc[2] += dot(dyt_ref[0], zs[...])

        @pl.when(part == TICKS - 1)
        def _():
            for b in range(4):
                rows = slice(OWN * b, OWN * b + OWN)
                cols = slice(LANES * b, LANES * b + LANES)
                for k in range(2):
                    p[chunk % 2, b % 2, b // 2, OWN * k : OWN * k + OWN] = acc[k, rows].astype(BF16)
                for i in range(4):
                    down = slice(OWN * i, OWN * i + OWN)
                    p[chunk % 2, b % 2, b // 2, 320:480, LANES * i : LANES * i + LANES] = acc[2, down, cols].astype(BF16)
            by_core(chunk).start()


def summed(dys, dyt, at, g, u, wd):
    n, d = dys.shape[1:]
    t = TOKENS_B
    last = CHUNKS * TICKS - 1
    steps = CHUNKS * TICKS + 3 * TICKS + 1

    def where(i):
        i = jnp.minimum(i, last)
        return 1 - i // (4 * TICKS), (i // TICKS) % 4, i % TICKS

    def spec(shape, pick):
        return pl.BlockSpec(shape, lambda i: pick(*where(i)))

    kept = spec((1, 1, t, WIDE), lambda l, c, k: (l, c, k, 0))
    wide = spec((1, d, t), lambda l, c, k: (l, 0, k))
    vmem = pl.BlockSpec(memory_space=pltpu.VMEM)
    return pl.pallas_call(
        sum_kernel,
        grid=(steps,),
        in_specs=[
            spec((1, t, d), lambda l, c, k: (l, k, 0)),
            wide,
            wide,
            kept,
            kept,
            spec((1, 4, 1, LANES, d), lambda l, c, k: (l, 0, c, 0, 0)),
        ],
        out_specs=[pl.BlockSpec(memory_space=pl.ANY), vmem],
        out_shape=[jax.ShapeDtypeStruct((CHUNKS, 2, 4, HALF, LANES), BF16), jax.ShapeDtypeStruct((8, LANES), F32)],
        scratch_shapes=[
            pltpu.VMEM((3, d, WIDE), F32),
            pltpu.VMEM((2, 2, 2, 480, WIDE), BF16),
            pltpu.VMEM((CHUNKS, 2, 480, WIDE), BF16),
            pltpu.VMEM((2, 2, 480, WIDE), BF16),
            pltpu.VMEM((CHUNKS, 480, WIDE), BF16),
            pltpu.VMEM((2, 2, 4, HALF, LANES), BF16),
            pltpu.VMEM((CHUNKS, 4, HALF, LANES), BF16),
            pltpu.VMEM((2, 4, HALF, LANES), BF16),
            pltpu.VMEM((CHUNKS, 3, HALF, LANES), BF16),
            pltpu.SemaphoreType.DMA((10, CHUNKS)),
            pltpu.SemaphoreType.DMA((10, CHUNKS)),
            *[pltpu.VMEM((TOKENS_B, WIDE), BF16)] * 3,
            pltpu.VMEM((4, 8, LANES), F32),
            pltpu.VMEM((3, 8, LANES), F32),
            pltpu.VMEM((3, 8, LANES), F32),
            pltpu.SemaphoreType.DMA((6,)),
            pltpu.SemaphoreType.DMA((6,)),
            pltpu.VMEM((CHUNKS, 2, 4, HALF, LANES), BF16),
            pltpu.SemaphoreType.DMA((CHUNKS,)),
        ],
        compiler_params=pltpu.CompilerParams(vmem_limit_bytes=LIMIT, collective_id=1, has_side_effects=True),
        cost_estimate=pl.CostEstimate(flops=16 * n * d * 2048, bytes_accessed=200_000_000, transcendentals=0),
        name="summed",
    )(dys, dyt, at, g, u, wd)


def adamw(w, m, v, g):
    m = 0.9 * m + 0.1 * g
    v = 0.95 * v + 0.05 * g * g
    step = m * lax.rsqrt(v + 1e-8) + 0.1 * w
    return (w - 0.02 * step).astype(BF16), m, v


def step_kernel(count, squares_ref, grad_ref, *refs):
    w, m, v, new_w, new_m, new_v = (refs[3 * i : 3 * i + 3] for i in range(6))
    squares = jnp.sum(jnp.sum(squares_ref[...], 0, keepdims=True), 1, keepdims=True)
    factor = jnp.minimum(1.0, 0.5 * lax.rsqrt(squares / count + 1e-30))
    half = pl.program_id(1)

    def apply(i, at, g):
        out = adamw(w[i][at].astype(F32), m[i][at], v[i][at], g.astype(F32) * factor)
        for ref, value in zip((new_w[i], new_m[i], new_v[i]), out, strict=True):
            ref[at] = value

    for c in range(4):
        for z in range(4):
            cols = slice(WIDE * z + LANES * c, WIDE * z + LANES * c + LANES)
            apply(0, (0, slice(None), cols), grad_ref[c, 0, z, pl.ds(pl.multiple_of(80 * half, 16), 80)])
            up_at = pl.ds(pl.multiple_of(OWN * (1 - half), 16), 80)
            apply(1, (0, slice(None), cols), grad_ref[c, half, z, up_at])
    for k in range(2):
        c = 2 * half + k
        turned = jnp.concatenate([grad_ref[c, 1, z, 80:HALF].astype(F32) for z in range(4)], 0).T
        apply(2, (0, slice(LANES * k, LANES * k + LANES)), turned)


def stepped(squares, grad, weights, m, v):
    layers, rows, f = weights[0].shape
    down = weights[2].shape[1:]
    a = pl.BlockSpec((1, rows // 2, f), lambda l, k: (l, k, 0))
    b = pl.BlockSpec((1, down[0] // 2, down[1]), lambda l, k: (l, k, 0))
    three = [a, a, b]
    shapes = [jax.ShapeDtypeStruct(w.shape, t) for t in (BF16, F32, F32) for w in weights]
    return pl.pallas_call(
        functools.partial(step_kernel, 4.0 * sum(w.size for w in weights)),
        grid=(layers, 2),
        in_specs=[
            pl.BlockSpec((8, LANES), lambda l, k: (0, 0)),
            pl.BlockSpec((4, 2, 4, HALF, LANES), lambda l, k: (1 - l, 0, 0, 0, 0)),
            *(three * 3),
        ],
        out_specs=three * 3,
        out_shape=shapes,
        compiler_params=pltpu.CompilerParams(vmem_limit_bytes=LIMIT),
        cost_estimate=pl.CostEstimate(flops=30_000_000, bytes_accessed=43_000_000, transcendentals=0),
        name="stepped",
    )(squares, grad, *weights, *m, *v)


def solution(mesh):
    def step(x, dy, *arrays):
        weights, m, v = (arrays[i : i + 3] for i in (0, 3, 6))
        h, at, g, u, wg, wu, wd = forward(x[0], *weights)
        dys, dyt, at, g, u = turn(h, dy[0], wg, wu, wd, at, g, u)
        grad, squares = summed(dys, dyt, at, g, u, wd.reshape(2, 4, 4, LANES, 640))
        return tuple(stepped(squares, grad, weights, m, v))

    states, cut = P(("rep", "r", "s"), None, None), P(None, "s", None)
    return jax.shard_map(
        step,
        mesh=mesh,
        in_specs=(states, states) + (cut,) * 9,
        out_specs=(P("rep", "s", None),) * 9,
        check_vma=False,
    )
```

```python
import functools

import jax
import jax.numpy as jnp
from jax import lax
from jax.experimental import pallas as pl
from jax.experimental.pallas import tpu as pltpu
from jax.sharding import PartitionSpec as P

F32, BF16 = jnp.float32, jnp.bfloat16
MESH = pl.DeviceIdType.MESH
LIMIT = 66_000_000
NT = (((1,), (1,)), ((), ()))
TOKENS_F, TOKENS_B = 512, 1024
LANES, WIDE, HALF, OWN = 128, 512, 240, 160
THREE = range(3)
STEPS_Z = (1, 2, 3)


def dot(a, b):
    return jnp.dot(a, b, preferred_element_type=F32)


def dot_nt(a, b):
    return lax.dot_general(a, b, NT, preferred_element_type=F32)


def sigmoid(g):
    return 0.5 * jnp.tanh(0.5 * g) + 0.5


def scale_of(wide):
    return lax.rsqrt(jnp.mean(wide * wide, -1, keepdims=True) + 1e-6)


def keep(ref, value, q):
    for c in range(4):
        ref[0, c, :, LANES * q : LANES * q + LANES] = value[:, LANES * c : LANES * c + LANES]


def forward_kernel(x_ref, g_block, u_block, d_block, h_ref, at_ref, g_ref, u_ref, wg_all, wu_all, wd_all, a_all, acc, *scratch):
    own, held, sems_s, sems_r, sems_own, sems_held = scratch[:3], scratch[3:6], *scratch[6:]
    q, tile, tiles = pl.program_id(0), pl.program_id(1), pl.num_programs(1)
    rep, r, s = lax.axis_index("rep"), lax.axis_index("r"), lax.axis_index("s")
    ax, core, ay, az = s // 2, s % 2, r // 4, r % 4
    mate = (rep, r, ax * 2 + 1 - core)
    far = (1 - ax) * 2 + core
    across = (rep, r, far)
    over = (rep, (1 - ay) * 4 + az, s)
    blocks, alls, halves = (g_block, u_block, d_block), (wg_all, wu_all, wd_all), (80, 80, 256)

    every = slice(None)
    groups = [[(0, i, slice(WIDE * n, WIDE * n + WIDE)) for i in range(2)] for n in range(4)]
    groups[0].append((0, 2, every))
    groups.append([(1, i, every) for i in THREE])
    order = [piece for group in groups for piece in group]

    def rows(i, place, which=None):
        n = halves[i]
        if which is None:
            return pl.ds(pl.multiple_of(2 * n * place, 16), 2 * n)
        return pl.ds(pl.multiple_of(2 * n * place + n * which, 16), n)

    def copy(kind, piece, src, dst, who):
        at = order.index(piece)
        return pltpu.make_async_remote_copy(
            src_ref=src, dst_ref=dst, send_sem=sems_s.at[kind, at], recv_sem=sems_r.at[kind, at], device_id=who, device_id_type=MESH
        )

    def there(piece, *place):
        layer, i, cols = piece
        return alls[i].at[layer, rows(i, *place), cols]

    def to_mate(piece):
        layer, i, cols = piece
        return copy(0, piece, blocks[i].at[layer, :, cols], there(piece, s), mate)

    def to_across(piece):
        layer, i, cols = piece
        return copy(1, piece, blocks[i].at[layer, rows(i, 0, ay), cols], there(piece, s, ay), across)

    def to_over(piece):
        return copy(2, piece, there(piece, far, ay), there(piece, far, ay), over)

    def near_on(piece):
        return copy(3, piece, there(piece, far, ay), there(piece, far, ay), mate)

    def far_on(piece):
        return copy(4, piece, there(piece, far, 1 - ay), there(piece, far, 1 - ay), mate)

    def own_in(i, layer):
        return pltpu.make_async_copy(blocks[i].at[layer], own[i].at[layer], sems_own.at[0, layer, i])

    def own_out(i, layer):
        return pltpu.make_async_copy(own[i].at[layer], alls[i].at[layer, rows(i, s)], sems_own.at[1, layer, i])

    def send(group):
        for piece in group:
            to_across(piece).start()
        for piece in group:
            to_mate(piece).start()

    def first_half(group):
        for piece in group:
            to_across(piece).wait_recv()
            to_over(piece).start()
            near_on(piece).start()

    def second_half(group):
        for piece in group:
            to_over(piece).wait_recv()
            far_on(piece).start()

    def finish(group):
        for piece in group:
            to_across(piece).wait_send()
            to_over(piece).wait_send()
            to_mate(piece).wait()
            near_on(piece).wait()
            far_on(piece).wait()

    def loads(n):
        return [
            pltpu.make_async_copy(alls[i].at[layer, :, cols], held[i] if i == 2 else held[i].at[n], sems_held.at[i, n])
            for layer, i, cols in groups[n]
        ]

    def when(n, t):
        return pl.when((q == n) & (tile == t))

    @when(0, 0)
    def _():
        for layer in range(2):
            for i in THREE:
                own_in(i, layer).start()
        barrier = pltpu.get_barrier_semaphore()
        for who in (mate, across, over):
            pl.semaphore_signal(barrier, inc=1, device_id=who, device_id_type=MESH)
        pl.semaphore_wait(barrier, 3)
        send(groups[0])
        for layer in range(2):
            for i in THREE:
                own_in(i, layer).wait()
                own_out(i, layer).start()
        first_half(groups[0])
        for n in STEPS_Z:
            send(groups[n])
        second_half(groups[0])
        finish(groups[0])
        for layer in range(2):
            for i in THREE:
                own_out(i, layer).wait()
        for load in loads(0):
            load.start()
        for load in loads(0):
            load.wait()

    @when(0, 1)
    def _():
        for n in STEPS_Z:
            first_half(groups[n])
        send(groups[4])

    for n in STEPS_Z:

        @when((n + 1) // 4, (n + 1) % 4)
        def _():
            second_half(groups[n])

    for n in STEPS_Z:

        @when(n - 1, 3)
        def _():
            finish(groups[n])
            for load in loads(n):
                load.start()

        @when(n, 0)
        def _():
            for load in loads(n):
                load.wait()

    @when(2, 0)
    def _():
        first_half(groups[4])

    @when(3, 2)
    def _():
        second_half(groups[4])

    @when(3, 3)
    def _():
        finish(groups[4])

    wg_ref, wu_ref, wd_ref = held
    n = x_ref.shape[0]
    here = pl.ds(pl.multiple_of(n * tile, n), n)

    @pl.when(q == 0)
    def _():
        wide = x_ref[...].astype(F32)
        a = (wide * scale_of(wide)).astype(BF16)
        a_all[here] = a
        at_ref[0] = a.T
        acc[here] = jnp.zeros_like(wide)

    for part in range(2):
        own_rows = pl.ds(pl.multiple_of(n * tile + n // 2 * part, n // 2), n // 2)
        some = slice(n // 2 * part, n // 2 * part + n // 2)
        a = a_all[own_rows]
        gate = dot(a, wg_ref[q])
        up = dot(a, wu_ref[q])
        for c in range(4):
            cols = slice(LANES * c, LANES * c + LANES)
            g_ref[0, c, some] = gate[:, cols]
            u_ref[0, c, some] = up[:, cols]
        z = (gate * sigmoid(gate) * up).astype(BF16)
        acc[own_rows] += dot(z, wd_ref[pl.ds(pl.multiple_of(WIDE * q, WIDE), WIDE)])

    @pl.when(q == 3)
    def _():
        h_ref[...] = (x_ref[...].astype(F32) + acc[here].astype(BF16).astype(F32)).astype(BF16)


def grads(gate, up, dz):
    s = sigmoid(gate)
    silu = gate * s
    dup = dz * silu
    dgate = dz * up * (s + silu * (1.0 - s))
    return silu * up, dgate, dup


def turn_kernel(h_ref, dy_ref, wg_ref, wu_ref, wd_ref, at_in, g_in, u_in, dys_ref, dyt_ref, at_ref, g_ref, u_ref, dg_ref, du_ref):
    wide = h_ref[...].astype(F32)
    scale = scale_of(wide)
    a = (wide * scale).astype(BF16)
    at_ref[0] = a.T
    dy = dy_ref[...]
    for q in range(4):
        cols = slice(WIDE * q, WIDE * q + WIDE)
        gate = dot(a, wg_ref[:, cols])
        up = dot(a, wu_ref[:, cols])
        dz = dot_nt(dy, wd_ref[cols, :]).astype(BF16).astype(F32)
        keep(g_ref, gate, q)
        keep(u_ref, up, q)
        _, dgate, dup = grads(gate, up, dz)
        dg_ref[:, cols] = dgate.astype(BF16)
        du_ref[:, cols] = dup.astype(BF16)
    da = dot_nt(dg_ref[...], wg_ref[...]) + dot_nt(du_ref[...], wu_ref[...])
    dot_mean = jnp.mean(da * wide, -1, keepdims=True)
    dh = da * scale - wide * (scale * scale * scale * dot_mean)
    dh = (dy.astype(F32) + dh).astype(BF16)
    dys_ref[1] = dy
    dys_ref[0] = dh
    dyt_ref[1] = dy.T
    dyt_ref[0] = dh.T


def forward(x, wg, wu, wd):
    n, d = x.shape
    f = wg.shape[2]
    t = TOKENS_B
    row = pl.BlockSpec((t, d), lambda q, i: (i, 0))
    kept = pl.BlockSpec((1, 4, t, LANES), lambda q, i: (0, 0, i, q))
    hbm = pl.BlockSpec(memory_space=pl.ANY)
    return pl.pallas_call(
        forward_kernel,
        grid=(4, n // t),
        in_specs=[row, hbm, hbm, hbm],
        out_specs=[
            pl.BlockSpec((t, d), lambda q, i: (jnp.where(q == 3, i, 0), 0)),
            pl.BlockSpec((1, d, t), lambda q, i: (0, 0, jnp.where(q == 0, i, n // t - 1))),
            kept,
            kept,
            hbm,
            hbm,
            hbm,
        ],
        out_shape=[
            jax.ShapeDtypeStruct((n, d), BF16),
            jax.ShapeDtypeStruct((2, d, n), BF16),
            jax.ShapeDtypeStruct((2, 4, n, f // 4), F32),
            jax.ShapeDtypeStruct((2, 4, n, f // 4), F32),
            jax.ShapeDtypeStruct((2, d, f), BF16),
            jax.ShapeDtypeStruct((2, d, f), BF16),
            jax.ShapeDtypeStruct((2, f, d), BF16),
        ],
        scratch_shapes=[
            pltpu.VMEM((n, d), BF16),
            pltpu.VMEM((n, d), F32),
            *[pltpu.VMEM(w.shape, BF16) for w in (wg, wu, wd)],
            *[pltpu.VMEM((4, d, WIDE), BF16)] * 2,
            pltpu.VMEM((f, d), BF16),
            pltpu.SemaphoreType.DMA((5, 12)),
            pltpu.SemaphoreType.DMA((5, 12)),
            pltpu.SemaphoreType.DMA((2, 2, 3)),
            pltpu.SemaphoreType.DMA((3, 4)),
        ],
        compiler_params=pltpu.CompilerParams(vmem_limit_bytes=LIMIT, collective_id=0, has_side_effects=True),
        cost_estimate=pl.CostEstimate(flops=6 * n * d * f, bytes_accessed=100_000_000, transcendentals=0),
        name="forward",
    )(x, wg, wu, wd)


def turn(h, dy, wg, wu, wd, at, g, u):
    n, d = h.shape
    f = wg.shape[2]
    t = TOKENS_F
    whole = lambda s: pl.BlockSpec((None, *s), lambda i: (1, 0, 0), pipeline_mode=pl.Buffered(1))
    row = pl.BlockSpec((t, d), lambda i: (i, 0))
    kept = pl.BlockSpec((1, 4, t, f // 4), lambda i: (1, 0, i, 0))
    hbm = pl.BlockSpec(memory_space=pl.ANY)
    return pl.pallas_call(
        turn_kernel,
        grid=(n // t,),
        in_specs=[row, row, whole((d, f)), whole((d, f)), whole((f, d)), hbm, hbm, hbm],
        out_specs=[
            pl.BlockSpec((2, t, d), lambda i: (0, i, 0)),
            pl.BlockSpec((2, d, t), lambda i: (0, 0, i)),
            pl.BlockSpec((1, d, t), lambda i: (1, 0, i)),
            kept,
            kept,
        ],
        out_shape=[
            jax.ShapeDtypeStruct((2, n, d), BF16),
            jax.ShapeDtypeStruct((2, d, n), BF16),
            jax.ShapeDtypeStruct((2, d, n), BF16),
            jax.ShapeDtypeStruct((2, 4, n, f // 4), F32),
            jax.ShapeDtypeStruct((2, 4, n, f // 4), F32),
        ],
        input_output_aliases={5: 2, 6: 3, 7: 4},
        scratch_shapes=[pltpu.VMEM((t, f), BF16)] * 2,
        compiler_params=pltpu.CompilerParams(vmem_limit_bytes=LIMIT),
        cost_estimate=pl.CostEstimate(flops=10 * n * d * f, bytes_accessed=100_000_000, transcendentals=0),
        name="turn",
    )(h, dy, wg, wu, wd, at, g, u)


TICKS = 4
PIECES = 4
t_b = TOKENS_B // PIECES
CHUNKS = 8


def sum_kernel(dys_ref, dyt_ref, at_ref, g_ref, u_ref, wd_ref, out_ref, sq_ref, acc, p, rc, q, rx, sy, ry, sz, rz, sems_s, sems_r, zs, dgs, dus, sqz, sqp, sqr, sq_s, sq_r, fin, fin_s):
    tick = pl.program_id(0)
    chunk, part = tick // TICKS, tick % TICKS
    rep, r, s = lax.axis_index("rep"), lax.axis_index("r"), lax.axis_index("s")
    x, core, y, z = s // 2, s % 2, r // 4, r % 4
    mate = (rep, r, x * 2 + 1 - core)
    across = (rep, r, (1 - x) * 2 + core)
    over = (rep, (1 - y) * 4 + z, s)
    others = [(rep, y * 4 + (z + k) % 4, s) for k in STEPS_Z]

    @pl.when(tick == 0)
    def _():
        barrier = pltpu.get_barrier_semaphore()
        for who in [mate, across, over, *others]:
            pl.semaphore_signal(barrier, inc=1, device_id=who, device_id_type=MESH)
        pl.semaphore_wait(barrier, 6)
        sq_ref[...] = jnp.zeros_like(sq_ref)

    def copy(src, dst, kind, j, who):
        return pltpu.make_async_remote_copy(
            src_ref=src, dst_ref=dst, send_sem=sems_s.at[kind, j], recv_sem=sems_r.at[kind, j], device_id=who, device_id_type=MESH
        )

    def by_core(j):
        return copy(p.at[j % 2, 1 - core], rc.at[j], 0, j, mate)

    def by_x(j, kept):
        which = y if kept else 1 - y
        return copy(q.at[j % 2, 1 - x, which], rx.at[j, which], 10 if kept else 1, j, across)

    def by_y(j):
        return copy(sy.at[j % 2, 1 - y], ry.at[j], 2, j, over)

    def by_z(j, k):
        return copy(sz.at[j % 2, (z + k) % 4], rz.at[j, k - 1], 2 + k, j, others[k - 1])

    def all_z(j, k):
        return copy(fin.at[j, y, z], fin.at[j, y, z], 5 + k, j, others[k - 1])

    def all_y(j):
        return copy(fin.at[j, y], fin.at[j, y], 9, j, over)

    def square(src, dst, kind, who):
        return pltpu.make_async_remote_copy(
            src_ref=src, dst_ref=dst, send_sem=sq_s.at[kind], recv_sem=sq_r.at[kind], device_id=who, device_id_type=MESH
        )

    def squares_z(k):
        return square(sqz.at[z], sqz.at[z], k - 1, others[k - 1])

    def squares(k):
        return square(sqp.at[k], sqr.at[k], 3 + k, (over, across, mate)[k])

    def give(j):
        return pltpu.make_async_copy(fin.at[j], out_ref.at[j], fin_s.at[j])

    def join_x(j, kept):
        which = y if kept else 1 - y
        by_x(j, kept).wait()
        total = (q[j % 2, x, which].astype(F32) + rx[j, which].astype(F32)).astype(BF16)
        for i in range(4):
            sy[j % 2, which, i] = total[:, LANES * i : LANES * i + LANES]

    def at(rounds, when, j_ok=True):
        j = chunk - rounds
        return j, (part == when) & (j >= 0) & (j < CHUNKS)

    j, now = at(1, 1)

    @pl.when(now)
    def _():
        by_core(j).wait()
        for k in range(2):
            q[j % 2, k] = (p[j % 2, core, k].astype(F32) + rc[j, k].astype(F32)).astype(BF16).reshape(2, HALF, WIDE)
        by_x(j, False).start()
        by_x(j, True).start()

    j, now = at(2, 0)

    @pl.when(now)
    def _():
        join_x(j, False)
        by_y(j).start()

    j, now = at(2, 1)

    @pl.when(now)
    def _():
        join_x(j, True)

    j, now = at(2, 2)

    @pl.when(now)
    def _():
        by_y(j).wait()
        sz[j % 2] = (sy[j % 2, y].astype(F32) + ry[j].astype(F32)).astype(BF16)
        for k in STEPS_Z:
            by_z(j, k).start()

    j, now = at(3, 0)

    @pl.when(now)
    def _():
        for k in STEPS_Z:
            by_z(j, k).wait()
        total = sz[j % 2, z].astype(F32)
        for k in THREE:
            total += rz[j, k].astype(F32)
        total = total.astype(BF16)
        fin[j, y, z] = total
        total = total.astype(F32)
        sq_ref[...] += jnp.sum((total * total).reshape(30, 8, LANES), 0)
        for k in STEPS_Z:
            all_z(j, k).start()

        @pl.when(j == CHUNKS - 1)
        def _():
            sqz[z] = sq_ref[...]
            for k in STEPS_Z:
                squares_z(k).start()

    j, now = at(3, 2)

    @pl.when(now)
    def _():
        for k in STEPS_Z:
            all_z(j, k).wait()
        all_y(j).start()

        @pl.when(j == CHUNKS - 1)
        def _():
            for k in STEPS_Z:
                squares_z(k).wait()
            total = (sqz[0] + sqz[1]) + (sqz[2] + sqz[3])
            for k in THREE:
                sqp[k] = total
                squares(k).start()
                squares(k).wait()
                total = total + sqr[k]
            sq_ref[...] = total

    j, now = at(4, 0)

    @pl.when(now)
    def _():
        all_y(j).wait()
        give(j).start()

    @pl.when(tick == pl.num_programs(0) - 1)
    def _():
        for j in range(CHUNKS):
            give(j).wait()

    @pl.when(chunk < CHUNKS)
    def _():
        @pl.when(part == 0)
        def _():
            acc[...] = jnp.zeros_like(acc)

        w = wd_ref[0, :, 0].reshape(WIDE, 640)
        for i in range(PIECES):
            rows = slice(t_b * i, t_b * i + t_b)
            dz = dot_nt(dys_ref[0, rows], w).astype(BF16).astype(F32)
            for ref, value in zip((zs, dgs, dus), grads(g_ref[0, 0, rows], u_ref[0, 0, rows], dz), strict=True):
                ref[rows] = value.astype(BF16)
        acc[0] += dot(at_ref[0], dgs[...])
        acc[1] += dot(at_ref[0], dus[...])
        acc[2] += dot(dyt_ref[0], zs[...])

        @pl.when(part == TICKS - 1)
        def _():
            for b in range(4):
                rows = slice(OWN * b, OWN * b + OWN)
                cols = slice(LANES * b, LANES * b + LANES)
                for k in range(2):
                    p[chunk % 2, b % 2, b // 2, OWN * k : OWN * k + OWN] = acc[k, rows].astype(BF16)
                for i in range(4):
                    down = slice(OWN * i, OWN * i + OWN)
                    p[chunk % 2, b % 2, b // 2, 320:480, LANES * i : LANES * i + LANES] = acc[2, down, cols].astype(BF16)
            by_core(chunk).start()


def summed(dys, dyt, at, g, u, wd):
    n, d = dys.shape[1:]
    t = TOKENS_B
    last = CHUNKS * TICKS - 1
    steps = CHUNKS * TICKS + 3 * TICKS + 1

    def where(i):
        i = jnp.minimum(i, last)
        return 1 - i // (4 * TICKS), (i // TICKS) % 4, i % TICKS

    def spec(shape, pick):
        return pl.BlockSpec(shape, lambda i: pick(*where(i)))

    kept = spec((1, 1, t, WIDE), lambda l, c, k: (l, c, k, 0))
    wide = spec((1, d, t), lambda l, c, k: (l, 0, k))
    vmem = pl.BlockSpec(memory_space=pltpu.VMEM)
    return pl.pallas_call(
        sum_kernel,
        grid=(steps,),
        in_specs=[
            spec((1, t, d), lambda l, c, k: (l, k, 0)),
            wide,
            wide,
            kept,
            kept,
            spec((1, 4, 1, LANES, d), lambda l, c, k: (l, 0, c, 0, 0)),
        ],
        out_specs=[pl.BlockSpec(memory_space=pl.ANY), vmem],
        out_shape=[jax.ShapeDtypeStruct((CHUNKS, 2, 4, HALF, LANES), BF16), jax.ShapeDtypeStruct((8, LANES), F32)],
        scratch_shapes=[
            pltpu.VMEM((3, d, WIDE), F32),
            pltpu.VMEM((2, 2, 2, 480, WIDE), BF16),
            pltpu.VMEM((CHUNKS, 2, 480, WIDE), BF16),
            pltpu.VMEM((2, 2, 2, HALF, WIDE), BF16),
            pltpu.VMEM((CHUNKS, 2, HALF, WIDE), BF16),
            pltpu.VMEM((2, 2, 4, HALF, LANES), BF16),
            pltpu.VMEM((CHUNKS, 4, HALF, LANES), BF16),
            pltpu.VMEM((2, 4, HALF, LANES), BF16),
            pltpu.VMEM((CHUNKS, 3, HALF, LANES), BF16),
            pltpu.SemaphoreType.DMA((11, CHUNKS)),
            pltpu.SemaphoreType.DMA((11, CHUNKS)),
            *[pltpu.VMEM((TOKENS_B, WIDE), BF16)] * 3,
            pltpu.VMEM((4, 8, LANES), F32),
            pltpu.VMEM((3, 8, LANES), F32),
            pltpu.VMEM((3, 8, LANES), F32),
            pltpu.SemaphoreType.DMA((6,)),
            pltpu.SemaphoreType.DMA((6,)),
            pltpu.VMEM((CHUNKS, 2, 4, HALF, LANES), BF16),
            pltpu.SemaphoreType.DMA((CHUNKS,)),
        ],
        compiler_params=pltpu.CompilerParams(vmem_limit_bytes=LIMIT, collective_id=1, has_side_effects=True),
        cost_estimate=pl.CostEstimate(flops=16 * n * d * 2048, bytes_accessed=200_000_000, transcendentals=0),
        name="summed",
    )(dys, dyt, at, g, u, wd)


def adamw(w, m, v, g):
    m = 0.9 * m + 0.1 * g
    v = 0.95 * v + 0.05 * g * g
    step = m * lax.rsqrt(v + 1e-8) + 0.1 * w
    return (w - 0.02 * step).astype(BF16), m, v


def step_kernel(count, squares_ref, grad_ref, *refs):
    w, m, v, new_w, new_m, new_v = (refs[3 * i : 3 * i + 3] for i in range(6))
    squares = jnp.sum(jnp.sum(squares_ref[...], 0, keepdims=True), 1, keepdims=True)
    factor = jnp.minimum(1.0, 0.5 * lax.rsqrt(squares / count + 1e-30))
    half = pl.program_id(1)

    def apply(i, at, g):
        out = adamw(w[i][at].astype(F32), m[i][at], v[i][at], g.astype(F32) * factor)
        for ref, value in zip((new_w[i], new_m[i], new_v[i]), out, strict=True):
            ref[at] = value

    for c in range(4):
        for z in range(4):
            cols = slice(WIDE * z + LANES * c, WIDE * z + LANES * c + LANES)
            apply(0, (0, slice(None), cols), grad_ref[c, 0, z, pl.ds(pl.multiple_of(80 * half, 16), 80)])
            up_at = pl.ds(pl.multiple_of(OWN * (1 - half), 16), 80)
            apply(1, (0, slice(None), cols), grad_ref[c, half, z, up_at])
    for k in range(2):
        c = 2 * half + k
        turned = jnp.concatenate([grad_ref[c, 1, z, 80:HALF].astype(F32) for z in range(4)], 0).T
        apply(2, (0, slice(LANES * k, LANES * k + LANES)), turned)


def stepped(squares, grad, weights, m, v):
    layers, rows, f = weights[0].shape
    down = weights[2].shape[1:]
    a = pl.BlockSpec((1, rows // 2, f), lambda l, k: (l, k, 0))
    b = pl.BlockSpec((1, down[0] // 2, down[1]), lambda l, k: (l, k, 0))
    three = [a, a, b]
    shapes = [jax.ShapeDtypeStruct(w.shape, t) for t in (BF16, F32, F32) for w in weights]
    return pl.pallas_call(
        functools.partial(step_kernel, 4.0 * sum(w.size for w in weights)),
        grid=(layers, 2),
        in_specs=[
            pl.BlockSpec((8, LANES), lambda l, k: (0, 0)),
            pl.BlockSpec((4, 2, 4, HALF, LANES), lambda l, k: (1 - l, 0, 0, 0, 0)),
            *(three * 3),
        ],
        out_specs=three * 3,
        out_shape=shapes,
        compiler_params=pltpu.CompilerParams(vmem_limit_bytes=LIMIT),
        cost_estimate=pl.CostEstimate(flops=30_000_000, bytes_accessed=43_000_000, transcendentals=0),
        name="stepped",
    )(squares, grad, *weights, *m, *v)


def solution(mesh):
    def step(x, dy, *arrays):
        weights, m, v = (arrays[i : i + 3] for i in (0, 3, 6))
        h, at, g, u, wg, wu, wd = forward(x[0], *weights)
        dys, dyt, at, g, u = turn(h, dy[0], wg, wu, wd, at, g, u)
        grad, squares = summed(dys, dyt, at, g, u, wd.reshape(2, 4, 4, LANES, 640))
        return tuple(stepped(squares, grad, weights, m, v))

    states, cut = P(("rep", "r", "s"), None, None), P(None, "s", None)
    return jax.shard_map(
        step,
        mesh=mesh,
        in_specs=(states, states) + (cut,) * 9,
        out_specs=(P("rep", "s", None),) * 9,
        check_vma=False,
    )
```
